32 devices in a mesh: grp: 4 (over y, x), bal: 8 (over z, core).
Axes of the slice: x: 2, y: 2, z: 4, core: 2. Of those that a mesh axis runs over, the one named last changes fastest.
Arguments:
- tracers: float32 [2, 64, 16, 2048], P(None, None, 'grp', 'bal'), may hold values from -6 to 6
- winds: bfloat16 [2, 64, 16, 2048], P(None, None, 'grp', 'bal'), may hold values from -16 to 16
- node_mass: float32 [16, 2048], P('grp', 'bal'), may hold values from 0.07 to 5.6
- column_cost: int32 [8, 1024], P('grp', 'bal'), may hold values from 1 to 3, as said below
- weight_in: bfloat16 [256, 1024], replicated, may hold values from -0.375 to 0.375
- weight_out: bfloat16 [1024, 256], replicated, may hold values from -0.1875 to 0.1875
Outputs:
- tracers_next: float32 [2, 64, 16, 2048], P(None, None, 'grp', 'bal')
- columns_out: bfloat16 [4, 64, 8, 1024], P(None, None, 'grp', 'bal')
The draws below stay inside these ranges and needn't reach their ends.
Inputs may be any that keep to these rules, and one draw needn't show every extreme that they name: `column_cost`: among the columns of one index of grp (rows 2 * g to 2 * g + 1 of all columns), exactly a quarter have cost 3 and exactly a quarter cost 2.
All inputs are finite; a program needn't handle non-finite values.
Results may differ from the reference program's by a relative error of at most 0.008.
Values may be sent and summed in bfloat16 or wider, within the bound.
A program may use at most 64 MiB of HBM per device.

```python
import math
import jax
import jax.numpy as jnp
from jax import lax

EX = 1
EY = 64
LEV = 64
HID = 1024
NEX = 4
NEY = 512
COLS = 256
N_GRP = 4
N_BAL = 8


def draw_column_cost(key, part):
    per_device = 4 * EX * EY
    members = per_device * N_BAL
    key_bias = jax.random.fold_in(key, 11)
    key_fine = jax.random.fold_in(key, 23)
    device_bias = jax.random.randint(key_bias, (N_GRP, N_BAL, 1), 0, 4)
    fine_bits = jax.random.randint(key_fine, (N_GRP, N_BAL, per_device), 0, 2048)
    position = jnp.arange(members, dtype=jnp.int32).reshape(1, N_BAL, per_device)
    scores = (device_bias * 2048 + fine_bits) * members + position
    flat_scores = scores.reshape(N_GRP, members)
    sorted_order = jnp.argsort(-flat_scores, axis=1)
    ranking = jnp.argsort(sorted_order, axis=1)
    costs_flat = jnp.where(ranking < members // 4, 3, jnp.where(ranking < members // 2, 2, 1)).astype(jnp.int32)
    blocks = costs_flat.reshape(N_GRP, N_BAL, 2 * EX, 2 * EY)
    return blocks.transpose(0, 2, 1, 3).reshape(N_GRP * 2 * EX, N_BAL * 2 * EY)


def draw_winds(key, part):
    layout = (2, LEV, 4 * NEX, 4 * NEY)
    key_sign = jax.random.fold_in(key, 101)
    key_size = jax.random.fold_in(key, 103)
    signs = jax.random.randint(key_sign, layout, 0, 2).astype(jnp.float32) * 2.0 - 1.0
    magnitude = jax.random.uniform(key_size, layout, jnp.float32, 10.0, 16.0)
    return (signs * magnitude).astype(jnp.bfloat16)


def draw_node_mass(key, part):
    key_flip = jax.random.fold_in(key, 201)
    key_elem = jax.random.fold_in(key, 203)
    key_node = jax.random.fold_in(key, 205)
    flip = jax.random.randint(key_flip, (), 0, 2)
    rows_idx = jnp.arange(NEX, dtype=jnp.int32)[:, None]
    cols_idx = jnp.arange(NEY, dtype=jnp.int32)[None, :]
    heavy = (rows_idx + cols_idx + flip) % 2 == 0
    spread = jax.random.uniform(key_elem, (NEX, NEY), jnp.float32, 0.0, 1.0)
    heavy_vals = 2.0 * jnp.exp(math.log(2.0) * spread)
    light_vals = 0.1 * jnp.exp(math.log(2.0) * spread)
    element_mass = jnp.where(heavy, heavy_vals, light_vals)
    expanded = jnp.repeat(jnp.repeat(element_mass, 4, axis=0), 4, axis=1)
    jitter = jnp.exp(jax.random.uniform(key_node, (4 * NEX, 4 * NEY), jnp.float32, math.log(0.7), math.log(1.4)))
    return (expanded * jitter).astype(jnp.float32)


def shard_levels(rng, extent, pieces, smallest, largest):
    factor_of = 1.0
    for dim, parts in pieces:
        steps = jax.random.uniform(jax.random.fold_in(jax.random.fold_in(rng, 6), dim), (parts,), jnp.float32, smallest / len(pieces), largest / len(pieces))
        factor_of = factor_of * jnp.repeat(jnp.exp(steps), extent[dim] // parts).reshape((-1,) + (1,) * (len(extent) - 1 - dim))
    return factor_of


def centred(own_key, dims, width, reach, shards=(), kind=jnp.bfloat16):
    level = shard_levels(own_key, dims, shards, -0.22, 0.18) if shards else 1.0
    values = jax.random.normal(own_key, dims, jnp.float32) * width * level
    return jnp.minimum(jnp.maximum(values, -reach), reach).astype(kind)


def setup_inputs(seed: int = 0) -> dict:
    keys = jax.random.split(jax.random.key(seed), 7)
    return {
        "tracers": centred(keys[0], (2, LEV, 4 * NEX, 4 * NEY), 1.0, 6.0, ((2, 4), (3, 8)), jnp.float32),
        "winds": draw_winds(jax.random.fold_in(keys[6], 71), 0),
        "node_mass": draw_node_mass(jax.random.fold_in(keys[6], 71), 0),
        "column_cost": draw_column_cost(jax.random.fold_in(keys[6], 71), 0),
        "weight_in": centred(keys[4], (4 * LEV, HID), (4 * LEV) ** -0.5, 0.375),
        "weight_out": centred(keys[5], (HID, 4 * LEV), HID ** -0.5, 0.1875),
    }


time_step = 0.02
remap_table = ((0.45, 0.4, 0.15, 0.0), (0.0, 0.15, 0.4, 0.45))
gll_points = (-1.0, -0.4472135954999579, 0.4472135954999579, 1.0)


def gll_matrix():
    matrix = []
    for row_idx in range(4):
        entries = []
        for col_idx in range(4):
            if row_idx == col_idx:
                running = 0.0
                for third_idx in range(4):
                    if third_idx != row_idx:
                        running += 1.0 / (gll_points[row_idx] - gll_points[third_idx])
                entries.append(2.0 * running)
            else:
                numerator = 1.0
                denominator = 1.0
                for third_idx in range(4):
                    if third_idx != row_idx:
                        numerator *= gll_points[row_idx] - gll_points[third_idx]
                    if third_idx != col_idx:
                        denominator *= gll_points[col_idx] - gll_points[third_idx]
                entries.append(2.0 * numerator / (denominator * (gll_points[row_idx] - gll_points[col_idx])))
        matrix.append(entries)
    return matrix


def derivatives(values):
    derivative = jnp.array(gll_matrix(), jnp.float32)
    layout = values.shape
    blocks_x = values.reshape(layout[:-2] + (layout[-2] // 4, 4, layout[-1]))
    along_x = jnp.einsum("ij,...ejy->...eiy", derivative, blocks_x, precision=lax.Precision.HIGHEST).reshape(layout)
    blocks_y = values.reshape(layout[:-1] + (layout[-1] // 4, 4))
    along_y = jnp.einsum("ij,...ej->...ei", derivative, blocks_y, precision=lax.Precision.HIGHEST).reshape(layout)
    return along_x, along_y


def tendency(tracer_vals, wind_vals):
    along_x, along_y = derivatives(tracer_vals)
    speeds = wind_vals.astype(jnp.float32)
    return -(speeds[0] * along_x + speeds[1] * along_y)


def assemble(values):
    layout = values.shape
    blocks = values.reshape(layout[:-2] + (layout[-2] // 4, 4, layout[-1]))
    first_edge = blocks[..., 0, :]
    last_edge = blocks[..., 3, :]
    new_first = first_edge + jnp.roll(last_edge, 1, axis=-2)
    new_last = last_edge + jnp.roll(first_edge, -1, axis=-2)
    blocks = jnp.concatenate([new_first[..., None, :], blocks[..., 1:3, :], new_last[..., None, :]], axis=-2)
    values = blocks.reshape(layout)
    blocks = values.reshape(layout[:-1] + (layout[-1] // 4, 4))
    first_edge = blocks[..., 0]
    last_edge = blocks[..., 3]
    new_first = first_edge + jnp.roll(last_edge, 1, axis=-1)
    new_last = last_edge + jnp.roll(first_edge, -1, axis=-1)
    blocks = jnp.concatenate([new_first[..., None], blocks[..., 1:3], new_last[..., None]], axis=-1)
    return blocks.reshape(layout)


def remap_columns(stacked):
    weights_table = jnp.array(remap_table, jnp.float32)
    layout = stacked.shape
    blocks = stacked.reshape(layout[:-2] + (layout[-2] // 4, 4, layout[-1] // 4, 4))
    cell_values = jnp.einsum("pa,qb,...xayb->...xpyq", weights_table, weights_table, blocks, precision=lax.Precision.HIGHEST)
    return cell_values.reshape(layout[:-2] + (layout[-2] // 2, layout[-1] // 2))


def network_step(column_state, weight_in, weight_out):
    hidden = jax.nn.gelu(jnp.dot(column_state.astype(jnp.bfloat16), weight_in, preferred_element_type=jnp.float32)).astype(jnp.bfloat16)
    return column_state + jnp.dot(hidden, weight_out, preferred_element_type=jnp.float32)


def blockwise(block_rows, weight_in, weight_out):
    blocks_count = block_rows.shape[0] // COLS
    mapped = lax.map(lambda one_block: network_step(one_block, weight_in, weight_out), block_rows.reshape(blocks_count, COLS, block_rows.shape[1]))
    return mapped.reshape(block_rows.shape)


def reference(tracers, winds, node_mass, column_cost, weight_in, weight_out):
    assembled = assemble(node_mass)

    def one_level(level_pair):
        tracer_level, wind_level = level_pair
        summed = assemble(tendency(tracer_level, wind_level) * node_mass)
        updated = tracer_level + time_step * (summed / assembled)
        stacked = jnp.concatenate([updated, wind_level.astype(jnp.float32)], axis=0)
        return updated, remap_columns(stacked).astype(jnp.bfloat16)

    by_level = (jnp.moveaxis(tracers, 1, 0), jnp.moveaxis(winds, 1, 0))
    updated, cell_values = lax.map(one_level, by_level)
    tracers_next = jnp.moveaxis(updated, 0, 1)
    cell_values = jnp.moveaxis(cell_values, 0, 1)
    features = cell_values.shape[0] * cell_values.shape[1]
    column_state = cell_values.reshape(features, -1).T.astype(jnp.float32)
    flat_cost = column_cost.reshape(-1)
    sorted_order = jnp.argsort(3 - flat_cost, stable=True)
    inverse = jnp.argsort(sorted_order, stable=True)
    column_state = column_state[sorted_order]
    everything = column_state.shape[0]
    for fraction in (1, 2, 4):
        leading = everything // fraction
        column_state = jnp.concatenate([blockwise(column_state[:leading], weight_in, weight_out), column_state[leading:]], axis=0)
    column_state = column_state[inverse].astype(jnp.bfloat16)
    columns_out = column_state.T.reshape(cell_values.shape)
    return tracers_next, columns_out
```

```python
import functools

import jax
import jax.numpy as jnp
import numpy as np
from jax import lax
from jax.experimental import pallas as pl
from jax.experimental.pallas import tpu as pltpu
from jax.sharding import PartitionSpec as P

MESH = pl.DeviceIdType.MESH
time_step = 0.02
remap_ints = ((9.0, 8.0, 3.0, 0.0), (0.0, 3.0, 8.0, 9.0))
gll_points = (-1.0, -0.4472135954999579, 0.4472135954999579, 1.0)

DIRS = ((1, 0), (-1, 0), (0, 1), (0, -1), (1, 1), (1, -1), (-1, 1), (-1, -1))
FROM_UP, FROM_DOWN, FROM_LEFT, FROM_RIGHT = 0, 1, 2, 3
FROM_UL, FROM_UR, FROM_DL, FROM_DR = 4, 5, 6, 7


def gll_matrix():
    points = gll_points
    matrix = np.zeros((4, 4))
    for i in range(4):
        for j in range(4):
            if i == j:
                matrix[i, i] = 2.0 * sum(
                    1.0 / (points[i] - points[k]) for k in range(4) if k != i
                )
            else:
                num = den = 1.0
                for k in range(4):
                    if k != i:
                        num *= points[i] - points[k]
                    if k != j:
                        den *= points[j] - points[k]
                matrix[i, j] = 2.0 * num / (den * (points[i] - points[j]))
    return matrix


def constants(across):
    elements = across // 4
    eye = np.eye(elements)
    along = np.kron(eye, gll_matrix().T).astype(np.float32)
    high = along.astype(jnp.bfloat16)
    low = (along - high.astype(np.float32)).astype(jnp.bfloat16)
    remap = np.kron(eye, np.array(remap_ints).T).astype(jnp.bfloat16)
    pick = np.zeros((4, 8, across), np.float32)
    for a in range(4):
        pick[a, a, 0] = 1.0
        pick[a, 4 + a, across - 1] = 1.0
    place = np.zeros((4, 48, across), np.float32)
    for a in range(4):
        place[a, 8 * 0 + 4 + a, 0] = 1.0
        place[a, 8 * 1 + a, across - 1] = 1.0
    place[0, 8 * 2 + 7, 0] = 1.0
    place[0, 8 * 3 + 3, across - 1] = 1.0
    place[3, 8 * 4 + 4, 0] = 1.0
    place[3, 8 * 5 + 0, across - 1] = 1.0
    return high, low, remap, pick.astype(jnp.bfloat16), place.astype(jnp.bfloat16)


def dot(a, b):
    return jnp.dot(a, b, preferred_element_type=jnp.float32)


def split(value):
    high = value.astype(jnp.bfloat16)
    return high, (value - high.astype(jnp.float32)).astype(jnp.bfloat16)


def kernel(
    sizes,
    tracers_ref, winds_ref, mass_ref, cost_ref, win_hbm, wout_hbm,
    dhigh_ref, dlow_ref, remap_ref, pick_ref, place_ref,
    next_ref, cols_ref,
    win, wout, win_t, wout_t, weighted, rows_out, rows_in, ends_out, ends_in,
    mass_in, state, local_sem, send_sem, recv_sem,
):
    n_grp, n_bal = sizes
    levels = winds_ref.shape[1] // 2
    across = winds_ref.shape[2]
    grp, bal = lax.axis_index("grp"), lax.axis_index("bal")

    def peer(i):
        dg, db = DIRS[i]
        return (lax.rem(grp + dg + n_grp, n_grp), lax.rem(bal + db + n_bal, n_bal))

    barrier = pltpu.get_barrier_semaphore()
    for i in range(8):
        pl.semaphore_signal(barrier, inc=1, device_id=peer(i), device_id_type=MESH)
    load_in = pltpu.make_async_copy(win_hbm, win, local_sem.at[0])
    load_out = pltpu.make_async_copy(wout_hbm, wout, local_sem.at[1])
    load_in.start()
    load_out.start()

    derivative = gll_matrix()

    def weigh(a):
        here = tracers_ref[a]
        high, low = split(here)
        along_y = dot(high, dhigh_ref[...]) + dot(low, dhigh_ref[...]) + dot(high, dlow_ref[...])
        along_x = sum(float(derivative[a, c]) * tracers_ref[c] for c in range(4))
        first = winds_ref[a, :levels, :].astype(jnp.float32)
        second = winds_ref[a, levels:, :].astype(jnp.float32)
        mass = mass_ref[a : a + 1, :]
        first, second = first * mass, second * mass
        for k in range(2):
            part = slice(k * levels, (k + 1) * levels)
            weighted[a, part, :] = -(first * along_x[part] + second * along_y[part])

    for a in (0, 3):
        weigh(a)
    rows_out[0] = weighted[3].astype(jnp.bfloat16)
    rows_out[1] = weighted[0].astype(jnp.bfloat16)

    pl.semaphore_wait(barrier, 8)
    copies = []

    def send(src, dst, slot, i):
        copy = pltpu.make_async_remote_copy(
            src_ref=src, dst_ref=dst, send_sem=send_sem.at[slot], recv_sem=recv_sem.at[slot],
            device_id=peer(i), device_id_type=MESH,
        )
        copy.start()
        copies.append(copy)
        return copy

    row_copies = [send(rows_out.at[i], rows_in.at[i], i, i) for i in range(2)]
    mass_copies = [send(mass_ref, mass_in.at[i], 2 + i, i) for i in range(8)]

    for a in (1, 2):
        weigh(a)
    ends = None
    for a in range(4):
        term = lax.dot_general(
            pick_ref[a], weighted[a].astype(jnp.bfloat16), (((1,), (1,)), ((), ())),
            preferred_element_type=jnp.float32,
        )
        ends = term if ends is None else ends + term
    ends_out[...] = ends

    lane = lax.broadcasted_iota(jnp.int32, (1, across), 1)
    takes_before = (lane % 4 == 0) & (lane > 0)
    takes_after = (lane % 4 == 3) & (lane < across - 1)

    half = across // 2
    winds_rows = 2 * levels
    for p in range(2):
        mixed = sum(
            remap_ints[p][a] * winds_ref[a].astype(jnp.float32)
            for a in range(4) if remap_ints[p][a]
        )
        high, low = split(mixed)
        cells = (dot(high, remap_ref[...]) + dot(low, remap_ref[...])) * (1.0 / 400.0)
        state[winds_rows:, p * half : (p + 1) * half] = cells.astype(jnp.bfloat16).astype(jnp.float32)

    end_copies = [send(ends_out, ends_in.at[i - 2], 8 + i, i) for i in range(2, 8)]

    load_in.wait()
    win_t[...] = win[...].T
    load_out.wait()
    wout_t[...] = wout[...].T

    for copy in mass_copies:
        copy.wait_recv()

    def join_rows(middle, upper, lower):
        return [middle[0:1] + upper[3:4], middle[1:2], middle[2:3], middle[3:4] + lower[0:1]]

    own = join_rows(mass_ref, mass_in[FROM_UP], mass_in[FROM_DOWN])
    left = join_rows(mass_in[FROM_LEFT], mass_in[FROM_UL], mass_in[FROM_DL])
    right = join_rows(mass_in[FROM_RIGHT], mass_in[FROM_UR], mass_in[FROM_DR])
    scales = []
    for a in range(4):
        before = pltpu.roll(jnp.where(lane == across - 1, left[a], own[a]), 1, 1)
        after = pltpu.roll(jnp.where(lane == 0, right[a], own[a]), across - 1, 1)
        total = own[a] + jnp.where(lane % 4 == 0, before, 0.0) + jnp.where(lane % 4 == 3, after, 0.0)
        scales.append(time_step / total)

    for copy in row_copies:
        copy.wait_recv()
    for copy in end_copies:
        copy.wait_recv()

    received = ends_in[...].reshape(48, ends_in.shape[-1]).astype(jnp.bfloat16)
    received = received.astype(jnp.float32).T.astype(jnp.bfloat16)
    mixed = [None, None]
    for a in range(4):
        value = weighted[a]
        if a == 0:
            value = value + rows_in[FROM_UP].astype(jnp.float32)
        if a == 3:
            value = value + rows_in[FROM_DOWN].astype(jnp.float32)
        before = pltpu.roll(value, 1, 1)
        after = pltpu.roll(value, across - 1, 1)
        total = value + jnp.where(takes_before, before, jnp.where(takes_after, after, 0.0))
        total = total + dot(received, place_ref[a])
        updated = tracers_ref[a] + scales[a] * total
        next_ref[a] = updated
        for p in range(2):
            if remap_ints[p][a]:
                term = remap_ints[p][a] * updated
                mixed[p] = term if mixed[p] is None else mixed[p] + term
    for p in range(2):
        high, low = split(mixed[p])
        cells = (dot(high, remap_ref[...]) + dot(low, remap_ref[...])) * (1.0 / 400.0)
        state[:winds_rows, p * half : (p + 1) * half] = cells.astype(jnp.bfloat16).astype(jnp.float32)

    cost = jnp.concatenate([cost_ref[0:1, :], cost_ref[1:2, :]], axis=1)
    hidden_size = win_t.shape[0]
    chunk = hidden_size // 4
    current = state[...]
    for step in range(3):
        inputs = current.astype(jnp.bfloat16)
        change = None
        for c in range(4):
            part = slice(c * chunk, (c + 1) * chunk)
            hidden = jax.nn.gelu(dot(win_t[part, :], inputs)).astype(jnp.bfloat16)
            term = dot(wout_t[:, part], hidden)
            change = term if change is None else change + term
        current = current + jnp.where(cost > step, change, 0.0)
    for p in range(2):
        cols_ref[p] = current[:, p * half : (p + 1) * half].astype(jnp.bfloat16)

    for copy in copies:
        copy.wait_send()


def shards(sizes, tracers, winds, node_mass, column_cost, weight_in, weight_out):
    levels, extent, across = tracers.shape[1:]
    features, hidden = weight_in.shape
    channels = 2 * levels
    rows = lambda x: x.transpose(2, 0, 1, 3).reshape(extent, channels, across)
    vmem = pl.BlockSpec(memory_space=pltpu.VMEM)
    hbm = pl.BlockSpec(memory_space=pl.ANY)
    f32, bf16 = jnp.float32, jnp.bfloat16
    next_rows, cols = pl.pallas_call(
        functools.partial(kernel, sizes),
        out_shape=(
            jax.ShapeDtypeStruct((extent, channels, across), f32),
            jax.ShapeDtypeStruct((2, features, across // 2), bf16),
        ),
        in_specs=[vmem] * 4 + [hbm] * 2 + [vmem] * 5,
        out_specs=(vmem, vmem),
        scratch_shapes=[
            pltpu.VMEM((features, hidden), bf16),
            pltpu.VMEM((hidden, features), bf16),
            pltpu.VMEM((hidden, features), bf16),
            pltpu.VMEM((features, hidden), bf16),
            pltpu.VMEM((extent, channels, across), f32),
            pltpu.VMEM((2, channels, across), bf16),
            pltpu.VMEM((2, channels, across), bf16),
            pltpu.VMEM((8, channels), f32),
            pltpu.VMEM((6, 8, channels), f32),
            pltpu.VMEM((8, extent, across), f32),
            pltpu.VMEM((features, across), f32),
            pltpu.SemaphoreType.DMA((2,)),
            pltpu.SemaphoreType.DMA((16,)),
            pltpu.SemaphoreType.DMA((16,)),
        ],
        compiler_params=pltpu.CompilerParams(collective_id=0, has_side_effects=True),
    )(
        rows(tracers), rows(winds), node_mass, column_cost, weight_in, weight_out,
        *constants(across),
    )
    tracers_next = next_rows.reshape(extent, 2, levels, across).transpose(1, 2, 0, 3)
    columns_out = cols.transpose(1, 0, 2).reshape(4, levels, 2, across // 2)
    return tracers_next, columns_out


def solution(mesh):
    grid = P(None, None, "grp", "bal")
    flat = P("grp", "bal")
    sizes = (mesh.shape["grp"], mesh.shape["bal"])
    return jax.shard_map(
        functools.partial(shards, sizes),
        mesh=mesh,
        in_specs=(grid, grid, flat, flat, P(), P()),
        out_specs=(grid, grid),
        check_vma=False,
    )
```

```python
import functools

import jax
import jax.numpy as jnp
import numpy as np
from jax import lax
from jax.experimental import pallas as pl
from jax.experimental.pallas import tpu as pltpu
from jax.sharding import PartitionSpec as P

MESH = pl.DeviceIdType.MESH
time_step = 0.02
remap_ints = ((9.0, 8.0, 3.0, 0.0), (0.0, 3.0, 8.0, 9.0))
gll_points = (-1.0, -0.4472135954999579, 0.4472135954999579, 1.0)

DIRS = ((1, 0), (-1, 0), (0, 1), (0, -1), (1, 1), (1, -1), (-1, 1), (-1, -1))
FROM_UP, FROM_DOWN, FROM_LEFT, FROM_RIGHT = 0, 1, 2, 3
FROM_UL, FROM_UR, FROM_DL, FROM_DR = 4, 5, 6, 7


def gll_matrix():
    points = gll_points
    matrix = np.zeros((4, 4))
    for i in range(4):
        for j in range(4):
            if i == j:
                matrix[i, i] = 2.0 * sum(
                    1.0 / (points[i] - points[k]) for k in range(4) if k != i
                )
            else:
                num = den = 1.0
                for k in range(4):
                    if k != i:
                        num *= points[i] - points[k]
                    if k != j:
                        den *= points[j] - points[k]
                matrix[i, j] = 2.0 * num / (den * (points[i] - points[j]))
    return matrix


def constants(across):
    elements = across // 4
    eye = np.eye(elements)
    along = np.kron(eye, gll_matrix().T).astype(np.float32)
    high = along.astype(jnp.bfloat16)
    low = (along - high.astype(np.float32)).astype(jnp.bfloat16)
    remap = np.kron(eye, np.array(remap_ints).T).astype(jnp.bfloat16)
    pick = np.zeros((4, 8, across), np.float32)
    for a in range(4):
        pick[a, a, 0] = 1.0
        pick[a, 4 + a, across - 1] = 1.0
    place = np.zeros((4, 48, across), np.float32)
    for a in range(4):
        place[a, 8 * 0 + 4 + a, 0] = 1.0
        place[a, 8 * 1 + a, across - 1] = 1.0
    place[0, 8 * 2 + 7, 0] = 1.0
    place[0, 8 * 3 + 3, across - 1] = 1.0
    place[3, 8 * 4 + 4, 0] = 1.0
    place[3, 8 * 5 + 0, across - 1] = 1.0
    return high, low, remap, pick.astype(jnp.bfloat16), place.astype(jnp.bfloat16)


def dot(a, b):
    return jnp.dot(a, b, preferred_element_type=jnp.float32)


def split(value):
    high = value.astype(jnp.bfloat16)
    return high, (value - high.astype(jnp.float32)).astype(jnp.bfloat16)


def kernel(
    sizes,
    tracers_hbm, winds_hbm, mass_hbm, cost_hbm, win_hbm, wout_hbm,
    dhigh_hbm, dlow_hbm, remap_hbm, pick_hbm, place_hbm,
    next_hbm, cols_ref,
    tracers_ref, winds_ref, mass_ref, cost_ref, win, wout,
    dhigh_ref, dlow_ref, remap_ref, pick_ref, place_ref,
    win_t, wout_t, weighted, next_ref, rows_out, rows_in, ends_out, ends_in,
    mass_in, local_sem, store_sem, send_sem, recv_sem,
):
    n_grp, n_bal = sizes
    levels, across = winds_ref.shape[1], winds_ref.shape[3]
    grp, bal = lax.axis_index("grp"), lax.axis_index("bal")

    def peer(i):
        dg, db = DIRS[i]
        return (lax.rem(grp + dg + n_grp, n_grp), lax.rem(bal + db + n_bal, n_bal))

    barrier = pltpu.get_barrier_semaphore()
    for i in range(8):
        pl.semaphore_signal(barrier, inc=1, device_id=peer(i), device_id_type=MESH)

    def load(src, dst, slot):
        copy = pltpu.make_async_copy(src, dst, local_sem.at[slot])
        copy.start()
        return copy

    load_rows = [load(tracers_hbm.at[:, :, a, :], tracers_ref.at[a], a) for a in range(4)]
    load_high = load(dhigh_hbm, dhigh_ref, 4)
    load_low = load(dlow_hbm, dlow_ref, 5)
    load_winds = load(winds_hbm, winds_ref, 6)
    load_mass = load(mass_hbm, mass_ref, 7)
    load_pick = load(pick_hbm, pick_ref, 8)
    load_remap = load(remap_hbm, remap_ref, 9)
    load_in = load(win_hbm, win, 10)
    load_out = load(wout_hbm, wout, 11)
    load_place = load(place_hbm, place_ref, 12)
    load_cost = load(cost_hbm, cost_ref, 13)
    for copy in (*load_rows, load_high, load_low, load_winds, load_mass):
        copy.wait()

    def tracer_row(a):
        return tracers_ref[a].reshape(2 * levels, across)

    derivative = gll_matrix()

    def weigh(a):
        here = tracer_row(a)
        high, low = split(here)
        along_y = dot(high, dhigh_ref[...]) + dot(low, dhigh_ref[...]) + dot(high, dlow_ref[...])
        along_x = sum(float(derivative[a, c]) * tracer_row(c) for c in range(4))
        first = winds_ref[0, :, a, :].astype(jnp.float32)
        second = winds_ref[1, :, a, :].astype(jnp.float32)
        mass = mass_ref[a : a + 1, :]
        first, second = first * mass, second * mass
        for k in range(2):
            part = slice(k * levels, (k + 1) * levels)
            weighted[a, part, :] = -(first * along_x[part] + second * along_y[part])

    for a in (0, 3):
        weigh(a)
    rows_out[0] = weighted[3].astype(jnp.bfloat16)
    rows_out[1] = weighted[0].astype(jnp.bfloat16)

    pl.semaphore_wait(barrier, 8)
    copies = []

    def send(src, dst, slot, i):
        copy = pltpu.make_async_remote_copy(
            src_ref=src, dst_ref=dst, send_sem=send_sem.at[slot], recv_sem=recv_sem.at[slot],
            device_id=peer(i), device_id_type=MESH,
        )
        copy.start()
        copies.append(copy)
        return copy

    row_copies = [send(rows_out.at[i], rows_in.at[i], i, i) for i in range(2)]
    mass_copies = [send(mass_ref, mass_in.at[i], 2 + i, i) for i in range(8)]

    for a in (1, 2):
        weigh(a)
    load_pick.wait()
    ends = None
    for a in range(4):
        term = lax.dot_general(
            pick_ref[a], weighted[a].astype(jnp.bfloat16), (((1,), (1,)), ((), ())),
            preferred_element_type=jnp.float32,
        )
        ends = term if ends is None else ends + term
    ends_out[...] = ends

    lane = lax.broadcasted_iota(jnp.int32, (1, across), 1)
    takes_before = (lane % 4 == 0) & (lane > 0)
    takes_after = (lane % 4 == 3) & (lane < across - 1)

    half = across // 2
    load_remap.wait()

    def cells_of(mixed):
        high, low = split(mixed)
        cells = (dot(high, remap_ref[...]) + dot(low, remap_ref[...])) * (1.0 / 400.0)
        return cells.astype(jnp.bfloat16).astype(jnp.float32)

    winds_cells = [
        [
            cells_of(sum(
                remap_ints[p][a] * winds_ref[k, :, a, :].astype(jnp.float32)
                for a in range(4) if remap_ints[p][a]
            ))
            for p in range(2)
        ]
        for k in range(2)
    ]

    end_copies = [send(ends_out, ends_in.at[i - 2], 8 + i, i) for i in range(2, 8)]

    load_in.wait()
    win_t[...] = win[...].T
    load_out.wait()
    wout_t[...] = wout[...].T

    for copy in mass_copies:
        copy.wait_recv()

    def join_rows(middle, upper, lower):
        return [middle[0:1] + upper[3:4], middle[1:2], middle[2:3], middle[3:4] + lower[0:1]]

    own = join_rows(mass_ref, mass_in[FROM_UP], mass_in[FROM_DOWN])
    left = join_rows(mass_in[FROM_LEFT], mass_in[FROM_UL], mass_in[FROM_DL])
    right = join_rows(mass_in[FROM_RIGHT], mass_in[FROM_UR], mass_in[FROM_DR])
    scales = []
    for a in range(4):
        before = pltpu.roll(jnp.where(lane == across - 1, left[a], own[a]), 1, 1)
        after = pltpu.roll(jnp.where(lane == 0, right[a], own[a]), across - 1, 1)
        total = own[a] + jnp.where(lane % 4 == 0, before, 0.0) + jnp.where(lane % 4 == 3, after, 0.0)
        scales.append(time_step / total)

    load_place.wait()
    load_cost.wait()
    for copy in row_copies:
        copy.wait_recv()
    for copy in end_copies:
        copy.wait_recv()

    received = ends_in[...].reshape(48, ends_in.shape[-1]).astype(jnp.bfloat16)
    received = received.astype(jnp.float32).T.astype(jnp.bfloat16)
    mixed = [None, None]
    stores = []
    for a in range(4):
        value = weighted[a]
        if a == 0:
            value = value + rows_in[FROM_UP].astype(jnp.float32)
        if a == 3:
            value = value + rows_in[FROM_DOWN].astype(jnp.float32)
        before = pltpu.roll(value, 1, 1)
        after = pltpu.roll(value, across - 1, 1)
        total = value + jnp.where(takes_before, before, jnp.where(takes_after, after, 0.0))
        total = total + dot(received, place_ref[a])
        updated = tracer_row(a) + scales[a] * total
        next_ref[a] = updated.reshape(2, levels, across)
        store = pltpu.make_async_copy(next_ref.at[a], next_hbm.at[:, :, a, :], store_sem.at[a])
        store.start()
        stores.append(store)
        for p in range(2):
            if remap_ints[p][a]:
                term = remap_ints[p][a] * updated
                mixed[p] = term if mixed[p] is None else mixed[p] + term
    current = jnp.concatenate(
        [
            jnp.concatenate([cells_of(mixed[p]) for p in range(2)], axis=1),
            jnp.concatenate(winds_cells[0], axis=1),
            jnp.concatenate(winds_cells[1], axis=1),
        ],
        axis=0,
    )

    cost = jnp.concatenate([cost_ref[0:1, :], cost_ref[1:2, :]], axis=1)
    hidden_size = win_t.shape[0]
    chunk = hidden_size // 4
    for step in range(3):
        inputs = current.astype(jnp.bfloat16)
        change = None
        for c in range(4):
            part = slice(c * chunk, (c + 1) * chunk)
            hidden = jax.nn.gelu(dot(win_t[part, :], inputs)).astype(jnp.bfloat16)
            term = dot(wout_t[:, part], hidden)
            change = term if change is None else change + term
        current = current + jnp.where(cost > step, change, 0.0)
    cols_ref[...] = jnp.stack([current[:, :half], current[:, half:]], axis=1).astype(jnp.bfloat16)

    for copy in stores:
        copy.wait()
    for copy in copies:
        copy.wait_send()


def shards(sizes, tracers, winds, node_mass, column_cost, weight_in, weight_out):
    levels, extent, across = tracers.shape[1:]
    features, hidden = weight_in.shape
    channels = 2 * levels
    vmem = pl.BlockSpec(memory_space=pltpu.VMEM)
    hbm = pl.BlockSpec(memory_space=pl.ANY)
    f32, bf16 = jnp.float32, jnp.bfloat16
    rows = (extent, 2, levels, across)
    tables = constants(across)
    tracers_next, cols = pl.pallas_call(
        functools.partial(kernel, sizes),
        out_shape=(
            jax.ShapeDtypeStruct(tracers.shape, f32),
            jax.ShapeDtypeStruct((features, 2, across // 2), bf16),
        ),
        in_specs=[hbm] * 11,
        out_specs=(hbm, vmem),
        scratch_shapes=[
            pltpu.VMEM(rows, f32),
            pltpu.VMEM(winds.shape, bf16),
            pltpu.VMEM(node_mass.shape, f32),
            pltpu.VMEM(column_cost.shape, jnp.int32),
            pltpu.VMEM((features, hidden), bf16),
            pltpu.VMEM((hidden, features), bf16),
            *[pltpu.VMEM(table.shape, bf16) for table in tables],
            pltpu.VMEM((hidden, features), bf16),
            pltpu.VMEM((features, hidden), bf16),
            pltpu.VMEM((extent, channels, across), f32),
            pltpu.VMEM(rows, f32),
            pltpu.VMEM((2, channels, across), bf16),
            pltpu.VMEM((2, channels, across), bf16),
            pltpu.VMEM((8, channels), f32),
            pltpu.VMEM((6, 8, channels), f32),
            pltpu.VMEM((8, extent, across), f32),
            pltpu.SemaphoreType.DMA((14,)),
            pltpu.SemaphoreType.DMA((4,)),
            pltpu.SemaphoreType.DMA((16,)),
            pltpu.SemaphoreType.DMA((16,)),
        ],
        compiler_params=pltpu.CompilerParams(collective_id=0, has_side_effects=True),
    )(tracers, winds, node_mass, column_cost, weight_in, weight_out, *tables)
    return tracers_next, cols.reshape(4, levels, 2, across // 2)


def solution(mesh):
    grid = P(None, None, "grp", "bal")
    flat = P("grp", "bal")
    sizes = (mesh.shape["grp"], mesh.shape["bal"])
    return jax.shard_map(
        functools.partial(shards, sizes),
        mesh=mesh,
        in_specs=(grid, grid, flat, flat, P(), P()),
        out_specs=(grid, grid),
        check_vma=False,
    )
```
